32 devices in a mesh: rep: 4 (over y, x), ep: 8 (over z, core).
Axes of the slice: x: 2, y: 2, z: 4, core: 2. Of those that a mesh axis runs over, the one named last changes fastest.
Arguments:
- hidden: bfloat16 [4, 1024, 2, 2048], P(None, ('rep', 'ep')), may hold values from -6 to 6
- out_grad: bfloat16 [4, 1024, 7168], P(None, ('rep', 'ep')), may hold values from -0.375 to 0.375
- route_weight: float32 [4, 1024, 2], P(None, ('rep', 'ep')), may hold values from 0.05 to 1
- expert_ids: int32 [4, 1024, 2], P(None, ('rep', 'ep')), may hold values from 0 to 7, as said below
Outputs:
- grad_down: bfloat16 [8, 2048, 7168], P('ep', None, 'rep')
- expert_load: float32 [8], replicated
The draws below stay inside these ranges and needn't reach their ends.
Inputs may be any that keep to these rules, and one draw needn't show every extreme that they name: `expert_ids`: in each micro-batch the 32 tokens of one device (aligned blocks of 32 tokens) name no expert in more than 16 pairs, and some expert is named in exactly 16; the 2 experts of a token differ.
All inputs are finite; a program needn't handle non-finite values.
Results may differ from the reference program's by a relative error of at most 0.0049.
Values may be sent and summed in bfloat16 or wider, within the bound.
A program may use at most 192 MiB of HBM per device.

```python
import math
import jax
import jax.numpy as jnp
from jax import lax

D = 7168
FF = 2048
TOK_DEV = 32
MICRO = 4
TOPK = 2
SPECIALIST_COUNT = 8
TOKENS = 1024
CAP = 16
N_REP = 4
N_EP = 8


def dispatched_specialist_group(group_seed_value, position_affinity_boost, position_specialist_pick):
    slot_total = SPECIALIST_COUNT * CAP
    noise_key, forced_key, order_key, turn_key = jax.random.split(group_seed_value, 4)
    gaussian_perturbation = jax.random.randint(noise_key, (slot_total,), 0, 65536, dtype=jnp.int32)
    mandated_specialists = jax.random.randint(forced_key, (), 0, SPECIALIST_COUNT, dtype=jnp.int32)
    plain_affinity = jnp.where(position_specialist_pick == mandated_specialists, jnp.int32(262144), position_affinity_boost + gaussian_perturbation)
    score = plain_affinity * slot_total + jnp.arange(slot_total, dtype=jnp.int32)
    chosen = lax.top_k(score, TOK_DEV * TOPK)[1].astype(jnp.int32)
    ordered = jnp.sort(chosen)
    experts = (ordered // CAP).reshape(TOPK, TOK_DEV).T
    token_order = jax.random.permutation(order_key, TOK_DEV).astype(jnp.int32)
    experts = experts[token_order]
    turn = jax.random.randint(turn_key, (TOK_DEV,), 0, TOPK, dtype=jnp.int32)
    column = (jnp.arange(TOPK, dtype=jnp.int32)[None, :] + turn[:, None]) % TOPK
    return jnp.take_along_axis(experts, column, axis=1).astype(jnp.int32)


def draw_expert_ids(key, part):
    rank_key, group_seed_value = jax.random.split(jax.random.fold_in(key, 7101))
    specialist_ordering = jax.random.permutation(rank_key, SPECIALIST_COUNT).astype(jnp.int32)
    affinity_boost = specialist_ordering * 49152 // SPECIALIST_COUNT
    position_specialist_pick = jnp.arange(SPECIALIST_COUNT * CAP, dtype=jnp.int32) // CAP
    position_affinity_boost = affinity_boost[position_specialist_pick]
    block_total = MICRO * (TOKENS // TOK_DEV)
    group_seed_values = jax.random.split(group_seed_value, block_total)
    dispatched_specialists = jax.vmap(lambda lone_specialist: dispatched_specialist_group(lone_specialist, position_affinity_boost, position_specialist_pick))(group_seed_values)
    return dispatched_specialists.reshape(MICRO, TOKENS, TOPK).astype(jnp.int32)


def strengthened(drawn, own_key, source, target, parts, factor):
    owner, partner = [(jnp.arange(drawn.shape[position]) // (drawn.shape[position] // parts)).reshape([-1 if axis == position else 1 for axis in range(drawn.ndim)]) for position in (source, target)]
    chosen = jax.random.permutation(own_key, parts)[partner]
    strong = (owner == chosen) | (owner == (partner + parts // 2) % parts)
    return jnp.where(strong, factor * drawn, drawn)


def level_of(own_key, shape, cuts, least, top_value):
    def one(dim, blocks):
        steps = jax.random.uniform(jax.random.fold_in(jax.random.fold_in(own_key, 6), dim), (blocks,), jnp.float32, least / len(cuts), top_value / len(cuts))
        return jnp.repeat(jnp.exp(steps), shape[dim] // blocks).reshape((-1,) + (1,) * (len(shape) - dim - 1))

    gain = one(*cuts[0])
    for cut in cuts[1:]:
        gain = gain * one(*cut)
    return gain


def gaussian(key, shape, width, limit, pieces=(), held_as=jnp.bfloat16):
    array = jax.random.normal(key, shape, jnp.float32) * width
    if len(pieces) > 0:
        array = level_of(key, shape, pieces, -0.22, 0.18) * array
    return jnp.clip(array, min=-limit, max=limit).astype(held_as)


def bell_draw_with(own_key, shape, width, limit, cuts, heavy, kind=jnp.bfloat16):
    result = width * jax.random.normal(own_key, shape, jnp.float32)
    if cuts:
        result = result * level_of(own_key, shape, cuts, -0.22, 0.18)
    return jnp.clip(strengthened(result, jax.random.fold_in(own_key, 3), *heavy), -limit, limit).astype(kind)


def setup_inputs(seed: int = 0) -> dict:
    arg_keys = jax.random.split(jax.random.key(seed), 5)
    return {
        "hidden": gaussian(arg_keys[0], (MICRO, TOKENS, TOPK, FF), 1.0, 6.0, ((1, 32),)),
        "out_grad": bell_draw_with(arg_keys[1], (MICRO, TOKENS, D), ((MICRO * TOK_DEV * TOPK * N_REP) ** -0.5), 0.375, ((1, 32),), (1, 2, 32, 2.75)),
        "route_weight": jnp.clip(jnp.exp(math.log(1.0) - 2.9957323 * jax.random.uniform(arg_keys[2], (MICRO, TOKENS, TOPK), jnp.float32) ** level_of(arg_keys[2], (MICRO, TOKENS, TOPK), ((1, 32),), -0.2, 0.2)), 0.05, 1.0),
        "expert_ids": draw_expert_ids(jax.random.fold_in(arg_keys[4], 71), 0),
    }


def reference(hidden, out_grad, route_weight, expert_ids):
    scaled = (route_weight[:, :, :, None] * out_grad[:, :, None, :].astype(jnp.float32)).astype(jnp.bfloat16)
    pair_hidden = hidden.reshape(-1, FF)
    pair_grad = scaled.reshape(-1, D)
    flat_routes = expert_ids.reshape(-1)
    largest = MICRO * N_REP * N_EP * CAP

    def one_expert(expert):
        chosen = flat_routes == expert
        picked = jnp.nonzero(chosen, size=largest, fill_value=0)[0]
        usable = jnp.arange(largest) < jnp.sum(chosen.astype(jnp.int32))
        selected = jnp.where(usable[:, None], pair_hidden[picked], jnp.zeros((), hidden.dtype))
        product = lax.dot_general(selected, pair_grad[picked], (((0,), (0,)), ((), ())), preferred_element_type=jnp.float32)
        return product.astype(jnp.bfloat16)

    grad_down = lax.map(one_expert, jnp.arange(SPECIALIST_COUNT, dtype=jnp.int32))
    tallies = jnp.sum((flat_routes[:, None] == jnp.arange(SPECIALIST_COUNT, dtype=jnp.int32)[None, :]).astype(jnp.float32), axis=0)
    expert_load = tallies * (SPECIALIST_COUNT / (MICRO * TOKENS * TOPK))
    return grad_down, expert_load
```

```python
import functools

import jax
import jax.numpy as jnp
from jax import lax
from jax.experimental import pallas as pl
from jax.experimental.pallas import tpu as pltpu
from jax.sharding import PartitionSpec as P

MESH = pl.DeviceIdType.MESH
CORES = 2
VMEM_BYTES = 60 * 1024 * 1024


def kernel(dims, send_ref, meta_ref, grad_ref, out_ref, load_ref, hid, met, gra, acc, picked, done,
           sem_hs, sem_hf, sem_hr, sem_ms, sem_mf, sem_mr, sem_gs, sem_gr, sem_gup, sem_gdn, sem_gsib,
           sem_gz, sem_gc, sem_loc, sem_out):
    reps, owners, slots, tokens, width, columns, scale = dims
    chips = owners // CORES
    per_chip = reps * CORES
    rep = lax.axis_index("rep")
    own = lax.axis_index("ep")
    z = own // CORES
    core = lax.rem(own, CORES)
    sib = z * CORES + (1 - core)

    def place(r, e):
        return (e // CORES) * per_chip + r * CORES + lax.rem(e, CORES)

    def order(s):
        low = jnp.minimum(z, chips - 1 - z)
        near = s <= 2 * low
        dist = jnp.where(near, (s + 1) // 2, s - low)
        up = jnp.where(near, 1 - lax.rem(s, 2), jnp.where(z < chips - 1 - z, 1, 0))
        sign = 2 * up - 1
        return z + sign * dist, sign

    def remote(src, dst, send, recv, **where):
        return pltpu.make_async_remote_copy(
            src_ref=src, dst_ref=dst, send_sem=send, recv_sem=recv,
            device_id=where, device_id_type=MESH,
        )

    barrier = pltpu.get_barrier_semaphore()
    for k in range(1, owners):
        pl.semaphore_signal(barrier, inc=1, device_id={"ep": lax.rem(own + k, owners)}, device_id_type=MESH)
    for k in range(1, reps):
        pl.semaphore_signal(barrier, inc=1, device_id={"rep": lax.rem(rep + k, reps)}, device_id_type=MESH)
    pl.semaphore_wait(barrier, owners - 1 + reps - 1)

    here = place(rep, own)

    def rows(e):
        return send_ref.at[pl.ds(pl.multiple_of(e * slots, slots), slots)]

    def slot_rows(i, n=1):
        return hid.at[pl.ds(pl.multiple_of(i * slots, slots), n * slots)]

    def cols(r):
        return grad_ref.at[:, pl.ds(pl.multiple_of(r * columns, columns), columns)]

    def dispatch(k):
        e = lax.rem(own + k, owners)
        return (
            remote(meta_ref.at[e], met.at[here], sem_ms.at[k], sem_mr.at[here], ep=e),
            remote(rows(e), slot_rows(here), sem_hs.at[k], sem_hr.at[here], ep=e),
        )

    def forward(e, k, first):
        i = place(rep, e)
        to = lax.rem(rep + k, reps)
        m_src = meta_ref.at[own] if first else met.at[i]
        h_src = rows(own) if first else slot_rows(i)
        return (
            remote(m_src, met.at[i], sem_mf.at[e, k], sem_mr.at[i], rep=to),
            remote(h_src, slot_rows(i), sem_hf.at[e, k], sem_hr.at[i], rep=to),
        )

    def exchange(k):
        to = lax.rem(rep + k, reps)
        return remote(cols(to), gra.at[here], sem_gs.at[k], sem_gr.at[here], rep=to)

    def g_src(i, first):
        return cols(rep) if first else gra.at[i]

    def g_up(i, first=False):
        return remote(g_src(i, first), gra.at[i], sem_gup.at[i], sem_gz.at[i], ep=own + CORES)

    def g_down(i, first=False):
        return remote(g_src(i, first), gra.at[i], sem_gdn.at[i], sem_gz.at[i], ep=own - CORES)

    def g_sib(i, first=False):
        return remote(g_src(i, first), gra.at[i], sem_gsib.at[i], sem_gc.at[i], ep=sib)

    def spread(i, first=False):
        @pl.when(z < chips - 1)
        def _():
            g_up(i, first).start()

        @pl.when(z > 0)
        def _():
            g_down(i, first).start()

        g_sib(i, first).start()

    local = (
        pltpu.make_async_copy(meta_ref.at[own], met.at[here], sem_loc.at[0]),
        pltpu.make_async_copy(rows(own), slot_rows(here), sem_loc.at[1]),
        pltpu.make_async_copy(cols(rep), gra.at[here], sem_loc.at[2]),
    )
    for k in range(1, reps):
        exchange(k).start()
    for k in range(1, owners):
        for c in dispatch(k):
            c.start()
    for c in local:
        c.start()
    for k in range(1, reps):
        for c in forward(own, k, True):
            c.start()
    spread(here, True)

    def pass_on(e):
        i = place(rep, e)
        remote(met.at[i], met.at[i], sem_ms.at[0], sem_mr.at[i], ep=own).wait_recv()
        remote(slot_rows(i), slot_rows(i), sem_hs.at[0], sem_hr.at[i], ep=own).wait_recv()
        for k in range(1, reps):
            for c in forward(e, k, False):
                c.start()

    pass_on(sib)
    for k in range(1, reps):
        i = place(lax.rem(rep + k, reps), own)
        remote(gra.at[i], gra.at[i], sem_gs.at[0], sem_gr.at[i], ep=own).wait_recv()
        spread(i)

    def pass_chip(s, carry):
        chip, _ = order(s)
        for c in range(CORES):
            pass_on(chip * CORES + c)
        return carry

    lax.fori_loop(1, chips, pass_chip, 0)
    for c in local:
        c.wait()

    half = reps // 2
    group = half * CORES
    depth = group * slots
    tile = 256

    def step(s, first, last):
        chip, sign = order(s)
        for part in range(2):
            for j in range(half):
                r = part * half + j
                mine = chip * per_chip + r * CORES + core
                other = chip * per_chip + r * CORES + (1 - core)
                if not first:
                    remote(gra.at[mine], gra.at[mine], sem_gs.at[0], sem_gz.at[mine], ep=own).wait_recv()

                    @pl.when((sign < 0) & (z < chips - 1))
                    def _():
                        g_up(mine).start()

                    @pl.when((sign > 0) & (z > 0))
                    def _():
                        g_down(mine).start()

                    g_sib(mine).start()
            for j in range(half):
                r = part * half + j
                other = chip * per_chip + r * CORES + (1 - core)
                remote(gra.at[other], gra.at[other], sem_gs.at[0], sem_gc.at[other], ep=own).wait_recv()

                @pl.when(r != rep)
                def _():
                    for c in range(CORES):
                        i = chip * per_chip + r * CORES + c
                        remote(met.at[i], met.at[i], sem_ms.at[0], sem_mr.at[i], ep=own).wait_recv()
                        remote(slot_rows(i), slot_rows(i), sem_hs.at[0], sem_hr.at[i], ep=own).wait_recv()

            base = chip * per_chip + part * group

            def select(g, carry):
                info = met[base + g]
                row = lax.broadcasted_iota(jnp.int32, (slots, tokens), 0).astype(jnp.float32)
                hit = row == info[0:1, :]
                weight = jnp.sum(jnp.where(hit, info[1:2, :], 0.0), axis=1, keepdims=True)
                rows_g = jnp.dot(hit.astype(jnp.bfloat16), gra[base + g], preferred_element_type=jnp.float32)
                picked[pl.ds(pl.multiple_of(g * slots, slots), slots), :] = (weight * rows_g).astype(jnp.bfloat16)
                return carry

            lax.fori_loop(0, group, select, 0)

            def block(t, carry):
                at = pl.ds(pl.multiple_of(t * tile, tile), tile)
                lhs = hid[pl.ds(pl.multiple_of(base * slots, slots), depth), at]
                prod = lax.dot_general(lhs, picked[...], (((0,), (0,)), ((), ())), preferred_element_type=jnp.float32)
                if first and part == 0:
                    acc[at, :] = prod
                elif last and part == 1:
                    done[at, :] = (acc[at, :] + prod).astype(jnp.bfloat16)
                    pltpu.make_async_copy(done.at[at], out_ref.at[at], sem_out.at[t]).start()
                else:
                    acc[at, :] += prod
                return carry

            lax.fori_loop(0, width // tile, block, 0)

    step(0, True, chips == 1)

    def middle(s, carry):
        step(s, False, False)
        return carry

    lax.fori_loop(1, chips - 1, middle, 0)
    step(chips - 1, False, True)

    load_ref[...] = jnp.sum(met[...], axis=0) * scale

    for k in range(1, reps):
        exchange(k).wait_send()
    for k in range(1, owners):
        for c in dispatch(k):
            c.wait_send()

    def drain(e, carry):
        for k in range(1, reps):
            i = place(rep, e)
            to = lax.rem(rep + k, reps)
            remote(met.at[i], met.at[i], sem_mf.at[e, k], sem_mr.at[i], rep=to).wait_send()
            remote(slot_rows(i), slot_rows(i), sem_hf.at[e, k], sem_hr.at[i], rep=to).wait_send()
        chip = e // CORES

        @pl.when(lax.rem(e, CORES) == core)
        def _():
            for r in range(reps):
                i = chip * per_chip + r * CORES + core
                g_sib(i).wait_send()

                @pl.when((chip <= z) & (z < chips - 1))
                def _():
                    g_up(i).wait_send()

                @pl.when((chip >= z) & (z > 0))
                def _():
                    g_down(i).wait_send()

        return carry

    lax.fori_loop(0, owners, drain, 0)

    def flush(t, carry):
        at = pl.ds(pl.multiple_of(t * tile, tile), tile)
        pltpu.make_async_copy(done.at[at], out_ref.at[at], sem_out.at[t]).wait()
        return carry

    lax.fori_loop(0, width // tile, flush, 0)


def fused(hidden, out_grad, route_weight, expert_ids):
    micro_count, tokens_here, choices_per, hidden_width = hidden.shape
    model_width = out_grad.shape[2]
    replicas = lax.axis_size("rep")
    owners = lax.axis_size("ep")
    capacity = 2 * tokens_here * choices_per // owners
    columns = model_width // replicas
    pair_count = tokens_here * choices_per
    tokens = micro_count * tokens_here
    slots = micro_count * capacity
    devices = replicas * owners
    total = micro_count * tokens_here * devices * choices_per

    ids = expert_ids.reshape(micro_count, pair_count)
    expert_index = jnp.arange(owners, dtype=jnp.int32)
    matches = ids[:, :, None] == expert_index
    ones = matches.astype(jnp.bfloat16)
    before = (jnp.arange(pair_count)[:, None] > jnp.arange(pair_count)[None, :]).astype(jnp.bfloat16)
    earlier = jnp.einsum("pq,mqe->mpe", before, ones, preferred_element_type=jnp.float32)
    spot = earlier + (capacity * jnp.arange(micro_count, dtype=jnp.float32))[:, None, None]
    in_expert = jnp.sum(jnp.where(matches, spot, 0.0), axis=2)
    slot_of_pair = (ids * slots + in_expert.astype(jnp.int32)).reshape(micro_count * pair_count)
    selector = (jnp.arange(owners * slots, dtype=jnp.int32)[:, None] == slot_of_pair[None, :]).astype(jnp.bfloat16)
    send_hidden = jnp.dot(
        selector, hidden.reshape(micro_count * pair_count, hidden_width), preferred_element_type=jnp.float32
    ).astype(jnp.bfloat16)
    by_token = matches.reshape(tokens, choices_per, owners)
    spot_row = jnp.max(jnp.where(by_token, spot.reshape(tokens, choices_per, owners), -1.0), axis=1).T
    weight_row = jnp.sum(jnp.where(by_token, route_weight.reshape(tokens, choices_per, 1), 0.0), axis=1).T
    counts = jnp.sum(by_token.astype(jnp.float32), axis=(0, 1))
    count_row = jnp.broadcast_to(jnp.pad(counts, (0, tokens - owners))[None, :], (owners, tokens))
    meta = jnp.stack([spot_row, weight_row, count_row] + [jnp.zeros_like(spot_row)] * 5, axis=1)

    dims = (replicas, owners, slots, tokens, hidden_width, columns, owners / total)
    dma = pltpu.SemaphoreType.DMA
    result, load = pl.pallas_call(
        functools.partial(kernel, dims),
        out_shape=(
            jax.ShapeDtypeStruct((hidden_width, columns), jnp.bfloat16),
            jax.ShapeDtypeStruct((8, tokens), jnp.float32),
        ),
        in_specs=[pl.BlockSpec(memory_space=pl.ANY)] * 3,
        out_specs=(pl.BlockSpec(memory_space=pl.ANY), pl.BlockSpec(memory_space=pltpu.VMEM)),
        scratch_shapes=[
            pltpu.VMEM((devices * slots, hidden_width), jnp.bfloat16),
            pltpu.VMEM((devices, 8, tokens), jnp.float32),
            pltpu.VMEM((devices, tokens, columns), jnp.bfloat16),
            pltpu.VMEM((hidden_width, columns), jnp.float32),
            pltpu.VMEM((replicas // 2 * CORES * slots, columns), jnp.bfloat16),
            pltpu.VMEM((hidden_width, columns), jnp.bfloat16),
            dma((owners,)), dma((owners, replicas)), dma((devices,)),
            dma((owners,)), dma((owners, replicas)), dma((devices,)),
            dma((replicas,)), dma((devices,)), dma((devices,)), dma((devices,)), dma((devices,)),
            dma((devices,)), dma((devices,)), dma((3,)), dma((hidden_width // 256,)),
        ],
        compiler_params=pltpu.CompilerParams(
            collective_id=0, has_side_effects=True, vmem_limit_bytes=VMEM_BYTES
        ),
    )(send_hidden, meta, out_grad.reshape(tokens, model_width))
    return result.reshape(1, hidden_width, columns), load[2, :owners]


def body(hidden, out_grad, route_weight, expert_ids):
    micro_count, tokens_here, choices_per, hidden_width = hidden.shape
    model_width = out_grad.shape[2]
    replicas = lax.axis_size("rep")
    owners = lax.axis_size("ep")
    capacity = 2 * tokens_here * choices_per // owners
    column_width = model_width // replicas
    pair_count = tokens_here * choices_per
    slot_rows = owners * capacity
    slot_index = jnp.arange(slot_rows, dtype=jnp.int32)
    expert_index = jnp.arange(owners, dtype=jnp.int32)
    pair_loads = jnp.zeros((owners,), jnp.float32)
    contract_rows = (((0,), (0,)), ((), ()))
    hidden_stack = []
    grad_stack = []
    for micro_step in range(micro_count):
        route_ids = expert_ids[micro_step].reshape(pair_count)
        matches = (route_ids[:, None] == expert_index[None, :]).astype(jnp.int32)
        earlier = jnp.cumsum(matches, axis=0) - matches
        position = jnp.sum(earlier * matches, axis=1)
        slot_of_pair = route_ids * capacity + position
        selector = (slot_index[:, None] == slot_of_pair[None, :]).astype(jnp.bfloat16)
        pair_loads = pair_loads + jnp.sum(matches, axis=0).astype(jnp.float32)
        scaled = (
            route_weight[micro_step][:, :, None]
            * out_grad[micro_step][:, None, :].astype(jnp.float32)
        ).astype(jnp.bfloat16)
        scaled = scaled.reshape(pair_count, model_width)
        pair_hidden = hidden[micro_step].reshape(pair_count, hidden_width)
        send_hidden = jnp.dot(selector, pair_hidden, preferred_element_type=jnp.float32).astype(
            jnp.bfloat16
        )
        send_grad = jnp.dot(selector, scaled, preferred_element_type=jnp.float32).astype(
            jnp.bfloat16
        )
        owner_hidden, owner_grad = (
            lax.all_to_all(
                send_hidden.reshape(owners, capacity, hidden_width),
                "ep",
                split_axis=0,
                concat_axis=0,
                tiled=True,
            ),
            lax.all_to_all(
                send_grad.reshape(owners, capacity, model_width),
                "ep",
                split_axis=0,
                concat_axis=0,
                tiled=True,
            ),
        )
        hidden_stack.append(owner_hidden.reshape(slot_rows, hidden_width))
        grad_stack.append(owner_grad.reshape(slot_rows, model_width))
    all_rows = micro_count * slot_rows
    stacked_hidden = jnp.concatenate(hidden_stack, axis=0).reshape(1, all_rows, hidden_width)
    stacked_grad = jnp.concatenate(grad_stack, axis=0).reshape(1, all_rows, model_width)
    grad_blocks = lax.all_to_all(stacked_grad, "rep", split_axis=2, concat_axis=0, tiled=True)
    flat_grad = grad_blocks.reshape(replicas * all_rows, column_width)
    gradient = lax.dot_general(
        lax.all_gather(stacked_hidden.reshape(all_rows, hidden_width), "rep", axis=0, tiled=True),
        flat_grad,
        contract_rows,
        preferred_element_type=jnp.float32,
    )
    all_loads = lax.psum(pair_loads, ("rep", "ep"))
    expert_load = all_loads / float(micro_count * tokens_here * replicas * choices_per)
    return (gradient.astype(jnp.bfloat16).reshape(1, hidden_width, column_width), expert_load)


def solution(mesh):
    def plan(hidden, out_grad, route_weight, expert_ids):
        devices = mesh.shape["rep"] * mesh.shape["ep"]
        tokens = hidden.shape[0] * hidden.shape[1]
        columns = out_grad.shape[2] // mesh.shape["rep"]
        slots = 2 * tokens * hidden.shape[2] // mesh.shape["ep"]
        held = 2 * devices * (tokens * columns + slots * hidden.shape[3]) + 6 * hidden.shape[3] * columns
        run = fused if held < 0.85 * VMEM_BYTES else body
        return run(hidden, out_grad, route_weight, expert_ids)

    return jax.shard_map(
        plan,
        mesh=mesh,
        in_specs=(
            P(None, ("rep", "ep"), None, None),
            P(None, ("rep", "ep"), None),
            P(None, ("rep", "ep"), None),
            P(None, ("rep", "ep"), None),
        ),
        out_specs=(P("ep", None, "rep"), P()),
        check_vma=False,
    )
```

```python
import functools

import jax
import jax.numpy as jnp
from jax import lax
from jax.experimental import pallas as pl
from jax.experimental.pallas import tpu as pltpu
from jax.sharding import PartitionSpec as P

MESH = pl.DeviceIdType.MESH
CORES = 2
VMEM_BYTES = 52 * 1024 * 1024
KERNEL_BYTES = 44 * 1024 * 1024


def kernel(dims, aux_ref, hidden_ref, grad_ref, out_ref, load_ref, hid, met, gra, acc, picked, packed, table,
           sem_hs, sem_hf, sem_hr, sem_ms, sem_mf, sem_mr, sem_gs, sem_gr, sem_gup, sem_gdn, sem_gsib,
           sem_gz, sem_gc, sem_loc):
    reps, owners, slots, tokens, width, columns, micro, scale = dims
    chips = owners // CORES
    per_chip = reps * CORES
    rep = lax.axis_index("rep")
    own = lax.axis_index("ep")
    z = own // CORES
    core = lax.rem(own, CORES)
    sib = z * CORES + (1 - core)

    def place(r, e):
        return (e // CORES) * per_chip + r * CORES + lax.rem(e, CORES)

    def order(s):
        low = jnp.minimum(z, chips - 1 - z)
        near = s <= 2 * low
        dist = jnp.where(near, (s + 1) // 2, s - low)
        up = jnp.where(near, 1 - lax.rem(s, 2), jnp.where(z < chips - 1 - z, 1, 0))
        sign = 2 * up - 1
        return z + sign * dist, sign

    def remote(src, dst, send, recv, **where):
        return pltpu.make_async_remote_copy(
            src_ref=src, dst_ref=dst, send_sem=send, recv_sem=recv,
            device_id=where, device_id_type=MESH,
        )

    barrier = pltpu.get_barrier_semaphore()
    for k in range(1, owners):
        pl.semaphore_signal(barrier, inc=1, device_id={"ep": lax.rem(own + k, owners)}, device_id_type=MESH)
    for k in range(1, reps):
        pl.semaphore_signal(barrier, inc=1, device_id={"rep": lax.rem(rep + k, reps)}, device_id_type=MESH)
    pl.semaphore_wait(barrier, owners - 1 + reps - 1)

    here = place(rep, own)

    def rows(e):
        return packed.at[pl.ds(pl.multiple_of(e * slots, slots), slots)]

    def slot_rows(i, n=1):
        return hid.at[pl.ds(pl.multiple_of(i * slots, slots), n * slots)]

    def cols(r):
        return grad_ref.at[:, pl.ds(pl.multiple_of(r * columns, columns), columns)]

    def dispatch(k):
        e = lax.rem(own + k, owners)
        return (
            remote(table.at[e], met.at[here], sem_ms.at[k], sem_mr.at[here], ep=e),
            remote(rows(e), slot_rows(here), sem_hs.at[k], sem_hr.at[here], ep=e),
        )

    def forward(e, k):
        i = place(rep, e)
        to = lax.rem(rep + k, reps)
        return (
            remote(met.at[i], met.at[i], sem_mf.at[e, k], sem_mr.at[i], rep=to),
            remote(slot_rows(i), slot_rows(i), sem_hf.at[e, k], sem_hr.at[i], rep=to),
        )

    def exchange(k):
        to = lax.rem(rep + k, reps)
        return remote(cols(to), gra.at[here], sem_gs.at[k], sem_gr.at[here], rep=to)

    def g_src(i, first):
        return cols(rep) if first else gra.at[i]

    def g_up(i, first=False):
        return remote(g_src(i, first), gra.at[i], sem_gup.at[i], sem_gz.at[i], ep=own + CORES)

    def g_down(i, first=False):
        return remote(g_src(i, first), gra.at[i], sem_gdn.at[i], sem_gz.at[i], ep=own - CORES)

    def g_sib(i, first=False):
        return remote(g_src(i, first), gra.at[i], sem_gsib.at[i], sem_gc.at[i], ep=sib)

    def spread(i, first=False):
        @pl.when(z < chips - 1)
        def _():
            g_up(i, first).start()

        @pl.when(z > 0)
        def _():
            g_down(i, first).start()

        g_sib(i, first).start()

    local = pltpu.make_async_copy(cols(rep), gra.at[here], sem_loc.at[0])
    for k in range(1, reps):
        exchange(k).start()
    spread(here, True)
    local.start()

    ids = [aux_ref[k : k + 1, :] for k in range(2)]
    weights = [aux_ref[2 + k : 3 + k, :] for k in range(2)]
    expert = lax.broadcasted_iota(jnp.int32, (owners, tokens), 0).astype(jnp.float32)
    match = [expert == ids[k] for k in range(2)]
    taken = jnp.where(match[0] | match[1], 1.0, 0.0)
    before = lax.broadcasted_iota(jnp.int32, (tokens, tokens), 0)
    after = lax.broadcasted_iota(jnp.int32, (tokens, tokens), 1)
    per_micro = tokens // micro
    same = lax.div(before, per_micro) == lax.div(after, per_micro)
    tri = jnp.where(same & (before < after), 1.0, 0.0).astype(jnp.bfloat16)
    earlier = jnp.dot(taken.astype(jnp.bfloat16), tri, preferred_element_type=jnp.float32)
    step_of = lax.div(lax.broadcasted_iota(jnp.int32, (owners, tokens), 1), per_micro)
    spot = jnp.where(taken > 0.0, earlier + (step_of * (slots // micro)).astype(jnp.float32), -1.0)
    weight_of = jnp.where(match[0], weights[0], jnp.where(match[1], weights[1], 0.0))
    counts = jnp.broadcast_to(jnp.sum(taken, axis=1, keepdims=True), (owners, tokens))
    for e in range(owners):
        first_choice = jnp.where(match[0][e : e + 1, :], 1.0, 0.0)
        table[e, 0:1, :] = spot[e : e + 1, :]
        table[e, 1:2, :] = weight_of[e : e + 1, :]
        table[e, 2:3, :] = first_choice
        table[e, 3:8, :] = jnp.zeros((5, tokens), jnp.float32)
        table[e, 8:, :] = counts

    def pack(e):
        info = table[e]
        row = lax.broadcasted_iota(jnp.int32, (slots, tokens), 0).astype(jnp.float32)
        hit = row == info[0:1, :]
        one = hit & (info[2:3, :] > 0.0)
        two = hit & (info[2:3, :] == 0.0)
        both = jnp.dot(one.astype(jnp.bfloat16), hidden_ref[:, :width], preferred_element_type=jnp.float32)
        both += jnp.dot(two.astype(jnp.bfloat16), hidden_ref[:, width:], preferred_element_type=jnp.float32)
        return both.astype(jnp.bfloat16)

    hid[pl.ds(pl.multiple_of(here * slots, slots), slots), :] = pack(own)
    met[here] = table[own]

    def pack_and_send(k, carry):
        e = lax.rem(own + k, owners)
        packed[pl.ds(pl.multiple_of(e * slots, slots), slots), :] = pack(e)

        @pl.when(k > 1)
        def _():
            for c in dispatch(k - 1):
                c.start()

        return carry

    lax.fori_loop(1, owners, pack_and_send, 0)
    for k in range(1, reps):
        for c in forward(own, k):
            c.start()
    for c in dispatch(owners - 1):
        c.start()

    def pass_on(e):
        i = place(rep, e)
        remote(met.at[i], met.at[i], sem_ms.at[0], sem_mr.at[i], ep=own).wait_recv()
        remote(slot_rows(i), slot_rows(i), sem_hs.at[0], sem_hr.at[i], ep=own).wait_recv()
        for k in range(1, reps):
            for c in forward(e, k):
                c.start()

    pass_on(sib)
    for k in range(1, reps):
        i = place(lax.rem(rep + k, reps), own)
        remote(gra.at[i], gra.at[i], sem_gs.at[0], sem_gr.at[i], ep=own).wait_recv()
        spread(i)

    def pass_chip(s, carry):
        chip, _ = order(s)
        for c in range(CORES):
            pass_on(chip * CORES + c)
        return carry

    lax.fori_loop(1, chips, pass_chip, 0)
    local.wait()

    half = reps // 2
    tile = 256

    def step(s, first, last):
        chip, sign = order(s)
        parts = [(0, half), (half, half)]
        if last:
            parts = [(0, half)] + [(r, 1) for r in range(half, reps)]
        for start, count in parts:
            group = count * CORES
            depth = group * slots
            for r in range(start, start + count):
                mine = chip * per_chip + r * CORES + core
                if not first:
                    remote(gra.at[mine], gra.at[mine], sem_gs.at[0], sem_gz.at[mine], ep=own).wait_recv()

                    @pl.when((sign < 0) & (z < chips - 1))
                    def _():
                        g_up(mine).start()

                    @pl.when((sign > 0) & (z > 0))
                    def _():
                        g_down(mine).start()

                    g_sib(mine).start()
            for r in range(start, start + count):
                other = chip * per_chip + r * CORES + (1 - core)
                remote(gra.at[other], gra.at[other], sem_gs.at[0], sem_gc.at[other], ep=own).wait_recv()

                @pl.when(r != rep)
                def _():
                    for c in range(CORES):
                        i = chip * per_chip + r * CORES + c
                        remote(met.at[i], met.at[i], sem_ms.at[0], sem_mr.at[i], ep=own).wait_recv()
                        remote(slot_rows(i), slot_rows(i), sem_hs.at[0], sem_hr.at[i], ep=own).wait_recv()

            base = chip * per_chip + start * CORES

            def select(g, carry):
                info = met[base + g]
                row = lax.broadcasted_iota(jnp.int32, (slots, tokens), 0).astype(jnp.float32)
                hit = row == info[0:1, :]
                weight = jnp.sum(jnp.where(hit, info[1:2, :], 0.0), axis=1, keepdims=True)
                rows_g = jnp.dot(hit.astype(jnp.bfloat16), gra[base + g], preferred_element_type=jnp.float32)
                picked[pl.ds(pl.multiple_of(g * slots, slots), slots), :] = (weight * rows_g).astype(jnp.bfloat16)
                return carry

            lax.fori_loop(0, group, select, 0)

            def block(t, carry):
                at = pl.ds(pl.multiple_of(t * tile, tile), tile)
                lhs = hid[pl.ds(pl.multiple_of(base * slots, slots), depth), at]
                prod = lax.dot_general(lhs, picked[:depth, :], (((0,), (0,)), ((), ())), preferred_element_type=jnp.float32)
                if first and start == 0:
                    acc[at, :] = prod
                elif last and start + count == reps:
                    out_ref[at, :] = (acc[at, :] + prod).astype(jnp.bfloat16)
                else:
                    acc[at, :] += prod
                return carry

            lax.fori_loop(0, width // tile, block, 0)

    step(0, True, chips == 1)

    def middle(s, carry):
        step(s, False, False)
        return carry

    lax.fori_loop(1, chips - 1, middle, 0)
    step(chips - 1, False, True)

    load_ref[...] = jnp.sum(met[:, 8:, :], axis=0) * scale

    for k in range(1, reps):
        exchange(k).wait_send()
    for k in range(1, owners):
        for c in dispatch(k):
            c.wait_send()

    def drain(e, carry):
        for k in range(1, reps):
            i = place(rep, e)
            to = lax.rem(rep + k, reps)
            remote(met.at[i], met.at[i], sem_mf.at[e, k], sem_mr.at[i], rep=to).wait_send()
            remote(slot_rows(i), slot_rows(i), sem_hf.at[e, k], sem_hr.at[i], rep=to).wait_send()
        chip = e // CORES

        @pl.when(lax.rem(e, CORES) == core)
        def _():
            for r in range(reps):
                i = chip * per_chip + r * CORES + core
                g_sib(i).wait_send()

                @pl.when((chip <= z) & (z < chips - 1))
                def _():
                    g_up(i).wait_send()

                @pl.when((chip >= z) & (z > 0))
                def _():
                    g_down(i).wait_send()

        return carry

    lax.fori_loop(0, owners, drain, 0)


def fused(hidden, out_grad, route_weight, expert_ids):
    micro_count, tokens_here, choices_per, hidden_width = hidden.shape
    model_width = out_grad.shape[2]
    replicas = lax.axis_size("rep")
    owners = lax.axis_size("ep")
    capacity = 2 * tokens_here * choices_per // owners
    columns = model_width // replicas
    tokens = micro_count * tokens_here
    slots = micro_count * capacity
    devices = replicas * owners
    total = micro_count * tokens_here * devices * choices_per

    routes = jnp.concatenate(
        [
            expert_ids.reshape(tokens, choices_per).T.astype(jnp.float32),
            route_weight.reshape(tokens, choices_per).T,
        ],
        axis=0,
    )

    dims = (replicas, owners, slots, tokens, hidden_width, columns, micro_count, owners / total)
    dma = pltpu.SemaphoreType.DMA
    result, load = pl.pallas_call(
        functools.partial(kernel, dims),
        out_shape=(
            jax.ShapeDtypeStruct((hidden_width, columns), jnp.bfloat16),
            jax.ShapeDtypeStruct((owners, tokens), jnp.float32),
        ),
        in_specs=[pl.BlockSpec(memory_space=pltpu.VMEM)] * 2 + [pl.BlockSpec(memory_space=pl.ANY)],
        out_specs=(pl.BlockSpec(memory_space=pltpu.VMEM),) * 2,
        scratch_shapes=[
            pltpu.VMEM((devices * slots, hidden_width), jnp.bfloat16),
            pltpu.VMEM((devices, 8 + owners, tokens), jnp.float32),
            pltpu.VMEM((devices, tokens, columns), jnp.bfloat16),
            pltpu.VMEM((hidden_width, columns), jnp.float32),
            pltpu.VMEM((replicas // 2 * CORES * slots, columns), jnp.bfloat16),
            pltpu.VMEM((owners * slots, hidden_width), jnp.bfloat16),
            pltpu.VMEM((owners, 8 + owners, tokens), jnp.float32),
            dma((owners,)), dma((owners, replicas)), dma((devices,)),
            dma((owners,)), dma((owners, replicas)), dma((devices,)),
            dma((replicas,)), dma((devices,)), dma((devices,)), dma((devices,)), dma((devices,)),
            dma((devices,)), dma((devices,)), dma((1,)),
        ],
        compiler_params=pltpu.CompilerParams(
            collective_id=0, has_side_effects=True, vmem_limit_bytes=KERNEL_BYTES
        ),
    )(routes, hidden.reshape(tokens, choices_per * hidden_width), out_grad.reshape(tokens, model_width))
    return result.reshape(1, hidden_width, columns), load[:, 0]


def body(hidden, out_grad, route_weight, expert_ids):
    micro_count, tokens_here, choices_per, hidden_width = hidden.shape
    model_width = out_grad.shape[2]
    replicas = lax.axis_size("rep")
    owners = lax.axis_size("ep")
    capacity = 2 * tokens_here * choices_per // owners
    column_width = model_width // replicas
    pair_count = tokens_here * choices_per
    slot_rows = owners * capacity
    slot_index = jnp.arange(slot_rows, dtype=jnp.int32)
    expert_index = jnp.arange(owners, dtype=jnp.int32)
    pair_loads = jnp.zeros((owners,), jnp.float32)
    contract_rows = (((0,), (0,)), ((), ()))
    hidden_stack = []
    grad_stack = []
    for micro_step in range(micro_count):
        route_ids = expert_ids[micro_step].reshape(pair_count)
        matches = (route_ids[:, None] == expert_index[None, :]).astype(jnp.int32)
        earlier = jnp.cumsum(matches, axis=0) - matches
        position = jnp.sum(earlier * matches, axis=1)
        slot_of_pair = route_ids * capacity + position
        selector = (slot_index[:, None] == slot_of_pair[None, :]).astype(jnp.bfloat16)
        pair_loads = pair_loads + jnp.sum(matches, axis=0).astype(jnp.float32)
        scaled = (
            route_weight[micro_step][:, :, None]
            * out_grad[micro_step][:, None, :].astype(jnp.float32)
        ).astype(jnp.bfloat16)
        scaled = scaled.reshape(pair_count, model_width)
        pair_hidden = hidden[micro_step].reshape(pair_count, hidden_width)
        send_hidden = jnp.dot(selector, pair_hidden, preferred_element_type=jnp.float32).astype(
            jnp.bfloat16
        )
        send_grad = jnp.dot(selector, scaled, preferred_element_type=jnp.float32).astype(
            jnp.bfloat16
        )
        owner_hidden, owner_grad = (
            lax.all_to_all(
                send_hidden.reshape(owners, capacity, hidden_width),
                "ep",
                split_axis=0,
                concat_axis=0,
                tiled=True,
            ),
            lax.all_to_all(
                send_grad.reshape(owners, capacity, model_width),
                "ep",
                split_axis=0,
                concat_axis=0,
                tiled=True,
            ),
        )
        hidden_stack.append(owner_hidden.reshape(slot_rows, hidden_width))
        grad_stack.append(owner_grad.reshape(slot_rows, model_width))
    all_rows = micro_count * slot_rows
    stacked_hidden = jnp.concatenate(hidden_stack, axis=0).reshape(1, all_rows, hidden_width)
    stacked_grad = jnp.concatenate(grad_stack, axis=0).reshape(1, all_rows, model_width)
    grad_blocks = lax.all_to_all(stacked_grad, "rep", split_axis=2, concat_axis=0, tiled=True)
    flat_grad = grad_blocks.reshape(replicas * all_rows, column_width)
    gradient = lax.dot_general(
        lax.all_gather(stacked_hidden.reshape(all_rows, hidden_width), "rep", axis=0, tiled=True),
        flat_grad,
        contract_rows,
        preferred_element_type=jnp.float32,
    )
    all_loads = lax.psum(pair_loads, ("rep", "ep"))
    expert_load = all_loads / float(micro_count * tokens_here * replicas * choices_per)
    return (gradient.astype(jnp.bfloat16).reshape(1, hidden_width, column_width), expert_load)


def solution(mesh):
    def plan(hidden, out_grad, route_weight, expert_ids):
        devices = mesh.shape["rep"] * mesh.shape["ep"]
        tokens = hidden.shape[0] * hidden.shape[1]
        columns = out_grad.shape[2] // mesh.shape["rep"]
        slots = 2 * tokens * hidden.shape[2] // mesh.shape["ep"]
        held = 2 * devices * (tokens * columns + slots * hidden.shape[3]) + 6 * hidden.shape[3] * columns
        run = fused if held < 0.9 * VMEM_BYTES else body
        return run(hidden, out_grad, route_weight, expert_ids)

    return jax.shard_map(
        plan,
        mesh=mesh,
        in_specs=(
            P(None, ("rep", "ep"), None, None),
            P(None, ("rep", "ep"), None),
            P(None, ("rep", "ep"), None),
            P(None, ("rep", "ep"), None),
        ),
        out_specs=(P("ep", None, "rep"), P()),
        check_vma=False,
    )
```
